32 devices in a mesh: dp: 2 (over x), tp: 4 (over z), ep: 4 (over y, core).
Axes of the slice: x: 2, y: 2, z: 4, core: 2. Of those that a mesh axis runs over, the one named last changes fastest.
Arguments:
- tokens_in: bfloat16 [4096, 2048], P(('dp', 'ep', 'tp')), parts along dimension 0
- expert_ids: int32 [4096, 8], P(('dp', 'ep', 'tp')), parts along dimension 0
- router_gates: float32 [4096, 8], P(('dp', 'ep', 'tp')), parts along dimension 0
- w_gate: bfloat16 [128, 2048, 768], P('ep', None, 'tp')
- w_up: bfloat16 [128, 2048, 768], P('ep', None, 'tp')
- w_down: bfloat16 [128, 768, 2048], P('ep', 'tp')
Outputs:
- output: bfloat16 [4096, 2048], P(('dp', 'ep', 'tp')), parts along dimension 0
There are 2 independent parts. The reference program is written for one: setup_inputs(seed, part) draws one part's arguments, and reference() takes and returns one part's arrays. A program takes and returns all parts, laid end to end along the dimension named above; an argument that names none is the same for every part.
All inputs are finite; a program needn't handle non-finite values.
Results may differ from the reference program's by a relative error of at most 0.0012.
Values are sent between devices in bfloat16 or wider.
A program may use at most 1 GiB of HBM per device.

```python
import jax
import jax.numpy as jnp
from jax import lax

TOKENS = 2048
D = 2048
FF = 768
EXPERTS = 128
TOP = 8
GROUPS = 4
BLOCK_ROWS = 128

ROWS = TOKENS // GROUPS
LOCAL = EXPERTS // GROUPS
HALF = TOP // 2


def draw_routing(key):
    k_perm, k_shift, k_pick, k_cols = jax.random.split(key, 4)
    rank = jax.vmap(lambda sub_key: jax.random.permutation(sub_key, ROWS))(jax.random.split(k_perm, GROUPS))
    shifts = jax.random.randint(k_shift, (GROUPS, ROWS // GROUPS), 1, GROUPS)
    source = jnp.arange(GROUPS)[:, None]
    first = (source + rank % GROUPS) % GROUPS
    second = (first + jnp.take_along_axis(shifts, rank // GROUPS, axis=1)) % GROUPS
    shard_pair = jnp.stack([first, second], axis=-1)
    scores = jax.random.randint(k_pick, (GROUPS, ROWS, 2, LOCAL), 0, 1 << 20) * LOCAL + jnp.arange(LOCAL)
    picks = jnp.argsort(scores, axis=-1)[..., :HALF]
    expert_ids = (shard_pair[..., None] * LOCAL + picks).reshape(TOKENS, TOP)
    col_scores = jax.random.randint(k_cols, (TOKENS, TOP), 0, 1 << 20) * TOP + jnp.arange(TOP)
    col_order = jnp.argsort(col_scores, axis=-1)
    return jnp.take_along_axis(expert_ids, col_order, axis=1).astype(jnp.int32)


def setup_inputs(seed: int = 0, part: int = 0) -> dict:
    part_key = jax.random.fold_in(jax.random.key(seed), part)
    k_tok, k_route, k_gate = jax.random.split(part_key, 3)
    k_w1, k_w3, k_w2 = jax.random.split(jax.random.key(seed + 1), 3)
    tokens_in = jax.random.normal(k_tok, (TOKENS, D), jnp.float32).astype(jnp.bfloat16)
    expert_ids = draw_routing(k_route)
    router_gates = jax.random.uniform(k_gate, (TOKENS, TOP), jnp.float32, 0.5, 1.5)
    w_gate = (jax.random.normal(k_w1, (EXPERTS, D, FF), jnp.float32) * D ** -0.5).astype(jnp.bfloat16)
    w_up = (jax.random.normal(k_w3, (EXPERTS, D, FF), jnp.float32) * D ** -0.5).astype(jnp.bfloat16)
    w_down = (jax.random.normal(k_w2, (EXPERTS, FF, D), jnp.float32) * FF ** -0.5).astype(jnp.bfloat16)
    return {'tokens_in': tokens_in, 'expert_ids': expert_ids, 'router_gates': router_gates, 'w_gate': w_gate, 'w_up': w_up, 'w_down': w_down}


def reference(tokens_in, expert_ids, router_gates, w_gate, w_up, w_down):
    pair_count = TOKENS * TOP
    flat_exp = expert_ids.reshape(-1)
    sort_order = jnp.argsort(flat_exp, stable=True)
    sorted_exp = flat_exp[sort_order]
    counts = jnp.bincount(flat_exp, length=EXPERTS)
    starts = jnp.cumsum(counts) - counts
    padded = (counts + BLOCK_ROWS - 1) // BLOCK_ROWS * BLOCK_ROWS
    pad_ends = jnp.cumsum(padded)
    pad_starts = pad_ends - padded
    slot_dest = pad_starts[sorted_exp] + jnp.arange(pair_count) - starts[sorted_exp]
    block_count = (pair_count + BLOCK_ROWS - 1) // BLOCK_ROWS + EXPERTS
    slot_pair = jnp.full((block_count * BLOCK_ROWS,), -1, jnp.int32).at[slot_dest].set(sort_order.astype(jnp.int32))
    safe_pair = jnp.maximum(slot_pair, 0)
    slot_tok = (safe_pair // TOP).reshape(block_count, BLOCK_ROWS)
    slot_gate = jnp.where(slot_pair >= 0, router_gates.reshape(-1)[safe_pair], 0.0).reshape(block_count, BLOCK_ROWS)
    block_start = jnp.arange(block_count) * BLOCK_ROWS
    block_exp = jnp.minimum(jnp.sum(pad_ends[None, :] <= block_start[:, None], axis=1), EXPERTS - 1)

    def add_block(running, block):
        tok_ids, gate_vals, expert = block
        row_act = tokens_in[tok_ids]
        h_gate = jnp.dot(row_act, w_gate[expert], preferred_element_type=jnp.float32)
        h_up = jnp.dot(row_act, w_up[expert], preferred_element_type=jnp.float32)
        hidden = (jax.nn.silu(h_gate) * h_up).astype(jnp.bfloat16)
        out_rows = jnp.dot(hidden, w_down[expert], preferred_element_type=jnp.float32)
        return running.at[tok_ids].add(out_rows * gate_vals[:, None]), None

    total, ignored = lax.scan(add_block, jnp.zeros((TOKENS, D), jnp.float32), (slot_tok, slot_gate, block_exp))
    return total.astype(jnp.bfloat16)
```

```python
import jax
import jax.numpy as jnp
from jax import lax
from jax.experimental import pallas as pl
from jax.experimental.pallas import tpu as pltpu
from jax.sharding import PartitionSpec as P

TOKEN_AXES = ('dp', 'ep', 'tp')
GROUP_AXES = ('ep', 'tp')
MB = 192
NBUF = 4
LANES = 128


def _moe_kernel(n_tok, dim, ffp, n_exp, n_pairs,
                tok_ref, gate_ref, start_ref, x_hbm, wg_hbm, wu_hbm, w2_hbm, y_hbm,
                xf, xst, yacc, wbuf, w2buf, xe, xb, obuf, xsem, wsem, ysem):
    cbs = dim // LANES
    tile_rows = cbs * 8
    xc = xst.shape[1]
    n_xc = n_tok // xc

    def w_copies(e, slot):
        return (pltpu.make_async_copy(wg_hbm.at[e], wbuf.at[slot, pl.ds(0, ffp)], wsem.at[slot, 0]),
                pltpu.make_async_copy(wu_hbm.at[e], wbuf.at[slot, pl.ds(ffp, ffp)], wsem.at[slot, 1]),
                pltpu.make_async_copy(w2_hbm.at[e], w2buf.at[slot], wsem.at[slot, 2]))

    def x_copy(i, slot):
        return pltpu.make_async_copy(x_hbm.at[pl.ds(i * xc, xc)], xst.at[slot], xsem.at[slot])

    x_copy(0, 0).start()
    x_copy(1, 1).start()
    for e in range(NBUF - 1):
        for c in w_copies(e, e):
            c.start()

    zero = jnp.zeros((tile_rows, LANES), jnp.float32)

    def x_chunk(i, carry):
        slot = lax.rem(i, 2)
        x_copy(i, slot).wait()

        def conv(r, carry2):
            r16 = pl.multiple_of(r * 16, 16)
            row = pl.multiple_of((i * xc + r16) * cbs, 2 * tile_rows)
            for cb in range(cbs):
                v = xst[slot, pl.ds(r16, 16), pl.ds(cb * LANES, LANES)].astype(jnp.float32)
                xf[pl.ds(row + cb * 8, 8), :] = v[:8]
                xf[pl.ds(row + tile_rows + cb * 8, 8), :] = v[8:]
            yacc[pl.ds(row, tile_rows), :] = zero
            yacc[pl.ds(row + tile_rows, tile_rows), :] = zero
            return carry2

        lax.fori_loop(0, xc // 16, conv, 0)

        @pl.when(i + 2 < n_xc)
        def _():
            x_copy(i + 2, slot).start()
        return carry

    lax.fori_loop(0, n_xc, x_chunk, 0)

    def expert(e, carry):
        slot = lax.rem(e, NBUF)

        @pl.when(e + NBUF - 1 < n_exp)
        def _():
            for c in w_copies(e + NBUF - 1, lax.rem(e + NBUF - 1, NBUF)):
                c.start()

        first = start_ref[e]
        last = start_ref[e + 1]
        for c in w_copies(e, slot):
            c.wait()

        def block(b, carry2):
            base = first + b * MB
            n = jnp.minimum(last - base, MB)
            groups = (n + 7) // 8

            def gather(m, c3):
                row = pl.multiple_of(m * tile_rows, tile_rows)
                vals = []
                for k in range(8):
                    t = tok_ref[base + m * 8 + k]
                    src = (t >> 3) * tile_rows + (t & 7)
                    vals.append(xf[pl.ds(src, cbs, stride=8), :])
                for k in range(8):
                    xe[pl.ds(row + k, cbs, stride=8), :] = vals[k]
                return c3

            lax.fori_loop(0, groups, gather, 0)

            def conv(r, c3):
                row = pl.multiple_of(r * 2 * tile_rows, 2 * tile_rows)
                for cb in range(cbs):
                    v = jnp.concatenate([xe[pl.ds(row + cb * 8, 8), :],
                                         xe[pl.ds(row + tile_rows + cb * 8, 8), :]], axis=0)
                    xb[pl.ds(pl.multiple_of(r * 16, 16), 16), pl.ds(cb * LANES, LANES)] = v.astype(jnp.bfloat16)
                return c3

            lax.fori_loop(0, (n + 15) // 16, conv, 0)

            at = lax.dot_general(wbuf[slot], xb[...], (((1,), (1,)), ((), ())),
                                 preferred_element_type=jnp.float32)
            ht = jax.nn.silu(at[:ffp]) * at[ffp:]
            h = ht.T.astype(jnp.bfloat16)
            for nc in range(dim // 256):
                o = jnp.dot(h, w2buf[slot, :, pl.ds(nc * 256, 256)], preferred_element_type=jnp.float32)
                for rb in range(MB // 8):
                    for s in range(2):
                        obuf[pl.ds(rb * tile_rows + (nc * 2 + s) * 8, 8), :] = (
                            o[rb * 8:rb * 8 + 8, s * LANES:(s + 1) * LANES])

            def combine(m, c3):
                row = pl.multiple_of(m * tile_rows, tile_rows)
                dst, acc = [], []
                for k in range(8):
                    p = m * 8 + k
                    t = jnp.where(p < n, tok_ref[base + p], n_tok)
                    d = pl.multiple_of(t * cbs, cbs)
                    dst.append(d)
                    acc.append(yacc[pl.ds(d, cbs), :]
                               + obuf[pl.ds(row + k, cbs, stride=8), :] * gate_ref[base + p])
                for k in range(8):
                    yacc[pl.ds(dst[k], cbs), :] = acc[k]
                return c3

            lax.fori_loop(0, groups, combine, 0)
            return carry2

        lax.fori_loop(0, (last - first + MB - 1) // MB, block, 0)
        return carry

    lax.fori_loop(0, n_exp, expert, 0)
    out = pltpu.make_async_copy(yacc.at[pl.ds(0, n_tok * cbs)], y_hbm, ysem)
    out.start()
    out.wait()


def _moe(tok, gate, start, x, wgt, wut, w2):
    n_exp, ffp, dim = wgt.shape
    n_tok = x.shape[0]
    cbs = dim // LANES
    import functools
    smem = pl.BlockSpec(memory_space=pltpu.SMEM)
    hbm = pl.BlockSpec(memory_space=pl.ANY)
    return pl.pallas_call(
        functools.partial(_moe_kernel, n_tok, dim, ffp, n_exp, tok.shape[0]),
        out_shape=jax.ShapeDtypeStruct((n_tok * cbs, LANES), jnp.float32),
        in_specs=[smem, smem, smem, hbm, hbm, hbm, hbm],
        out_specs=hbm,
        scratch_shapes=[
            pltpu.VMEM((n_tok * cbs, LANES), jnp.float32),
            pltpu.VMEM((2, 128, dim), jnp.bfloat16),
            pltpu.VMEM(((n_tok + 8) * cbs, LANES), jnp.float32),
            pltpu.VMEM((NBUF, 2 * ffp, dim), jnp.bfloat16),
            pltpu.VMEM((NBUF, ffp, dim), jnp.bfloat16),
            pltpu.VMEM((MB * cbs, LANES), jnp.float32),
            pltpu.VMEM((MB, dim), jnp.bfloat16),
            pltpu.VMEM((MB * cbs, LANES), jnp.float32),
            pltpu.SemaphoreType.DMA((2,)),
            pltpu.SemaphoreType.DMA((NBUF, 3)),
            pltpu.SemaphoreType.DMA,
        ],
        compiler_params=pltpu.CompilerParams(vmem_limit_bytes=62 * 1024 * 1024),
        cost_estimate=pl.CostEstimate(flops=20_000_000_000, bytes_accessed=100_000_000, transcendentals=1_000_000),
    )(tok, gate, start, x, wgt, wut, w2)


def _routing(ids, gates, local_count, first_expert):
    devs, choices, rows = ids.shape
    n_tok = devs * rows
    tok = (lax.broadcasted_iota(jnp.int32, ids.shape, 0) * rows
           + lax.broadcasted_iota(jnp.int32, ids.shape, 2))
    local = ids - first_expert
    key = jnp.where((local >= 0) & (local < local_count), local * n_tok + tok, local_count * n_tok)
    key = key.reshape(-1)
    n_pairs = key.shape[0] // 4
    bounds = jnp.arange(local_count + 1, dtype=jnp.int32) * n_tok
    start = jnp.sum((key[None, :] < bounds[:, None]).astype(jnp.int32), axis=1)
    key_s, gate_s = lax.sort((key, gates.reshape(-1)), num_keys=1, is_stable=False)
    tok_s = key_s[:n_pairs + MB] & (n_tok - 1)
    return tok_s, gate_s[:n_pairs + MB], start


def solution(mesh):
    def expert_block(tok_shard, id_shard, gate_shard, w_gate, w_up, w_down):
        x = lax.all_gather(tok_shard, GROUP_AXES, axis=0, tiled=True)
        meta = jnp.concatenate([id_shard.T.astype(jnp.float32), gate_shard.T], axis=0)
        meta = lax.all_gather(meta, GROUP_AXES, axis=0)
        choices = id_shard.shape[1]
        ids = meta[:, :choices].astype(jnp.int32)
        gates = meta[:, choices:]
        local_count = w_gate.shape[0]
        tok, gate, start = _routing(ids, gates, local_count, lax.axis_index('ep') * local_count)
        y = _moe(tok, gate, start, x, jnp.swapaxes(w_gate, 1, 2), jnp.swapaxes(w_up, 1, 2), w_down)
        y = lax.psum_scatter(y, GROUP_AXES, scatter_dimension=0, tiled=True)
        return y.reshape(tok_shard.shape).astype(jnp.bfloat16)

    return jax.shard_map(
        expert_block,
        mesh=mesh,
        in_specs=(P(TOKEN_AXES, None), P(TOKEN_AXES, None), P(TOKEN_AXES, None),
                  P('ep', None, 'tp'), P('ep', None, 'tp'), P('ep', 'tp', None)),
        out_specs=P(TOKEN_AXES, None),
        check_vma=False,
    )
```

```python
import functools

import jax
import jax.numpy as jnp
from jax import lax
from jax.experimental import pallas as pl
from jax.experimental.pallas import tpu as pltpu
from jax.sharding import PartitionSpec as P

TOKEN_AXES = ('dp', 'ep', 'tp')
GROUP_AXES = ('ep', 'tp')
MB = 192
NBUF = 4
LANES = 128


def _moe_kernel(n_tok, dim, ffp, n_exp, n_pairs,
                tok_ref, gate_ref, start_ref, x_hbm, wg_hbm, wu_hbm, w2_hbm, y_hbm,
                xf, xst, yacc, wbuf, w2buf, xe, xb, obuf, xsem, wsem, ysem):
    cbs = dim // LANES
    tile_rows = cbs * 8
    xc = xst.shape[1]
    n_xc = n_tok // xc

    def w_copies(e, slot):
        return (pltpu.make_async_copy(wg_hbm.at[e], wbuf.at[slot, pl.ds(0, ffp)], wsem.at[slot, 0]),
                pltpu.make_async_copy(wu_hbm.at[e], wbuf.at[slot, pl.ds(ffp, ffp)], wsem.at[slot, 1]),
                pltpu.make_async_copy(w2_hbm.at[e], w2buf.at[slot], wsem.at[slot, 2]))

    def x_copy(i, slot):
        return pltpu.make_async_copy(x_hbm.at[pl.ds(i * xc, xc)], xst.at[slot], xsem.at[slot])

    x_copy(0, 0).start()
    x_copy(1, 1).start()
    for e in range(NBUF - 1):
        for c in w_copies(e, e):
            c.start()

    zero = jnp.zeros((tile_rows, LANES), jnp.float32)

    def x_chunk(i, carry):
        slot = lax.rem(i, 2)
        x_copy(i, slot).wait()

        def conv(r, carry2):
            r16 = pl.multiple_of(r * 16, 16)
            row = pl.multiple_of((i * xc + r16) * cbs, 2 * tile_rows)
            for cb in range(cbs):
                v = xst[slot, pl.ds(r16, 16), pl.ds(cb * LANES, LANES)].astype(jnp.float32)
                xf[pl.ds(row + cb * 8, 8), :] = v[:8]
                xf[pl.ds(row + tile_rows + cb * 8, 8), :] = v[8:]
            yacc[pl.ds(row, tile_rows), :] = zero
            yacc[pl.ds(row + tile_rows, tile_rows), :] = zero
            return carry2

        lax.fori_loop(0, xc // 16, conv, 0)

        @pl.when(i + 2 < n_xc)
        def _():
            x_copy(i + 2, slot).start()
        return carry

    lax.fori_loop(0, n_xc, x_chunk, 0)

    def expert(e, carry):
        slot = lax.rem(e, NBUF)

        @pl.when(e + NBUF - 1 < n_exp)
        def _():
            for c in w_copies(e + NBUF - 1, lax.rem(e + NBUF - 1, NBUF)):
                c.start()

        first = start_ref[e]
        last = start_ref[e + 1]
        for c in w_copies(e, slot):
            c.wait()

        def block(b, carry2):
            base = first + b * MB
            n = jnp.minimum(last - base, MB)
            groups = (n + 7) // 8

            def gather(m, c3):
                row = pl.multiple_of(m * tile_rows, tile_rows)
                vals = []
                for k in range(8):
                    t = tok_ref[base + m * 8 + k]
                    src = (t >> 3) * tile_rows + (t & 7)
                    vals.append(xf[pl.ds(src, cbs, stride=8), :])
                for k in range(8):
                    xe[pl.ds(row + k, cbs, stride=8), :] = vals[k]
                return c3

            lax.fori_loop(0, groups, gather, 0)

            def conv(r, c3):
                row = pl.multiple_of(r * 2 * tile_rows, 2 * tile_rows)
                for cb in range(cbs):
                    v = jnp.concatenate([xe[pl.ds(row + cb * 8, 8), :],
                                         xe[pl.ds(row + tile_rows + cb * 8, 8), :]], axis=0)
                    xb[pl.ds(pl.multiple_of(r * 16, 16), 16), pl.ds(cb * LANES, LANES)] = v.astype(jnp.bfloat16)
                return c3

            lax.fori_loop(0, (n + 15) // 16, conv, 0)

            at = lax.dot_general(wbuf[slot], xb[...], (((1,), (1,)), ((), ())),
                                 preferred_element_type=jnp.float32)
            ht = jax.nn.silu(at[:ffp]) * at[ffp:]
            h = ht.T.astype(jnp.bfloat16)
            for nc in range(dim // 256):
                o = jnp.dot(h, w2buf[slot, :, pl.ds(nc * 256, 256)], preferred_element_type=jnp.float32)
                for rb in range(MB // 8):
                    for s in range(2):
                        obuf[pl.ds(rb * tile_rows + (nc * 2 + s) * 8, 8), :] = (
                            o[rb * 8:rb * 8 + 8, s * LANES:(s + 1) * LANES])

            def combine(m, c3):
                row = pl.multiple_of(m * tile_rows, tile_rows)
                dst, acc = [], []
                for k in range(8):
                    p = m * 8 + k
                    t = jnp.where(p < n, tok_ref[base + p], n_tok)
                    d = pl.multiple_of(t * cbs, cbs)
                    dst.append(d)
                    acc.append(yacc[pl.ds(d, cbs), :]
                               + obuf[pl.ds(row + k, cbs, stride=8), :] * gate_ref[base + p])
                for k in range(8):
                    yacc[pl.ds(dst[k], cbs), :] = acc[k]
                return c3

            lax.fori_loop(0, groups, combine, 0)
            return carry2

        lax.fori_loop(0, (last - first + MB - 1) // MB, block, 0)
        return carry

    lax.fori_loop(0, n_exp, expert, 0)
    out = pltpu.make_async_copy(yacc.at[pl.ds(0, n_tok * cbs)], y_hbm, ysem)
    out.start()
    out.wait()


def _moe(tok, gate, start, x, wgt, wut, w2):
    n_exp, ffp, dim = wgt.shape
    n_tok = x.shape[0]
    cbs = dim // LANES
    smem = pl.BlockSpec(memory_space=pltpu.SMEM)
    hbm = pl.BlockSpec(memory_space=pl.ANY)
    return pl.pallas_call(
        functools.partial(_moe_kernel, n_tok, dim, ffp, n_exp, tok.shape[0]),
        out_shape=jax.ShapeDtypeStruct((n_tok * cbs, LANES), jnp.float32),
        in_specs=[smem, smem, smem, hbm, hbm, hbm, hbm],
        out_specs=hbm,
        scratch_shapes=[
            pltpu.VMEM((n_tok * cbs, LANES), jnp.float32),
            pltpu.VMEM((2, 128, dim), jnp.bfloat16),
            pltpu.VMEM(((n_tok + 8) * cbs, LANES), jnp.float32),
            pltpu.VMEM((NBUF, 2 * ffp, dim), jnp.bfloat16),
            pltpu.VMEM((NBUF, ffp, dim), jnp.bfloat16),
            pltpu.VMEM((MB * cbs, LANES), jnp.float32),
            pltpu.VMEM((MB, dim), jnp.bfloat16),
            pltpu.VMEM((MB * cbs, LANES), jnp.float32),
            pltpu.SemaphoreType.DMA((2,)),
            pltpu.SemaphoreType.DMA((NBUF, 3)),
            pltpu.SemaphoreType.DMA,
        ],
        compiler_params=pltpu.CompilerParams(vmem_limit_bytes=62 * 1024 * 1024),
        cost_estimate=pl.CostEstimate(flops=20_000_000_000, bytes_accessed=100_000_000, transcendentals=1_000_000),
    )(tok, gate, start, x, wgt, wut, w2)


def _routing(ids, gates, local_count, first_expert):
    devs, choices, rows = ids.shape
    n_tok = devs * rows
    tok = (lax.broadcasted_iota(jnp.int32, ids.shape, 0) * rows
           + lax.broadcasted_iota(jnp.int32, ids.shape, 2))
    local = ids - first_expert
    key = jnp.where((local >= 0) & (local < local_count), local * n_tok + tok, local_count * n_tok)
    key = key.reshape(-1)
    n_pairs = key.shape[0] // 4
    bounds = jnp.arange(local_count + 1, dtype=jnp.int32) * n_tok
    start = jnp.sum((key[None, :] < bounds[:, None]).astype(jnp.int32), axis=1)
    key_s, gate_s = lax.sort((key, gates.reshape(-1)), num_keys=1, is_stable=False)
    tok_s = key_s[:n_pairs + MB] & (n_tok - 1)
    return tok_s, gate_s[:n_pairs + MB], start


def _wire(ep, tp):
    return ep // 2, ep % 2


def _remote(src, dst, send, recv, ep, tp):
    return pltpu.make_async_remote_copy(src_ref=src, dst_ref=dst, send_sem=send, recv_sem=recv,
                                        device_id={'ep': ep, 'tp': tp},
                                        device_id_type=pl.DeviceIdType.MESH)


def _gather_kernel(tps, x_ref, meta_ref, xall, mall, buf, ms, mr, zs, zr, ys, yr, cs, cr, ls):
    ep, tp = lax.axis_index('ep'), lax.axis_index('tp')
    n_dev = mall.shape[0]
    y, c = ep // 2, ep % 2
    me = ep * tps + tp
    partner = y * 2 + (1 - c)
    across = (1 - y) * 2 + c

    barrier = pltpu.get_barrier_semaphore()
    for k in range(1, n_dev):
        peer = (me + k) % n_dev
        pl.semaphore_signal(barrier, inc=1, device_id={'ep': peer // tps, 'tp': peer % tps},
                            device_id_type=pl.DeviceIdType.MESH)
    pl.semaphore_wait(barrier, n_dev - 1)

    metas = []
    for k in range(1, n_dev):
        peer = (me + k) % n_dev
        cp = _remote(meta_ref, mall.at[me], ms.at[k], mr.at[k], peer // tps, peer % tps)
        cp.start()
        metas.append(cp)
    mall[pl.ds(me, 1)] = meta_ref[...][None]

    def body(z):
        sends = []

        def send(b, src, kind, ep_to, tp_to):
            s, r = {'r': (zs, zr), 'l': (zs, zr), 'y': (ys, yr), 'c': (cs, cr)}[kind]
            zi = b[1]
            si = {'r': zi, 'l': tps + zi, 'y': zi, 'c': b[0] * tps + zi}[kind]
            row = (b[0] if kind != 'c' else b[0])
            idx = block(b)
            cp = _remote(src, buf.at[idx], s.at[si], r.at[zi if kind in 'rly' else si], ep_to, tp_to)
            cp.start()
            sends.append(cp)

        def block(b):
            yy = y if b[0] == 0 else 1 - y
            return (yy * 2 + c) * tps + b[1]

        def keep(idx, src, n):
            cp = pltpu.make_async_copy(src, xall.at[idx], ls.at[n])
            cp.start()
            locals_.append(cp)

        locals_ = []
        own = block((0, z))
        if z < tps - 1:
            send((0, z), x_ref, 'r', ep, z + 1)
        if z > 0:
            send((0, z), x_ref, 'l', ep, z - 1)
        send((0, z), x_ref, 'y', across, z)
        send((0, z), x_ref, 'c', partner, z)
        keep(own, x_ref, 0)

        events = []
        order = [z]
        for dist in range(1, tps):
            if z - dist >= 0:
                events.append((dist * 2, 'L', z - dist))
                order.append(z - dist)
            if z + dist < tps:
                events.append((dist * 2, 'R', z + dist))
                order.append(z + dist)
        for i, zi in enumerate(order):
            events.append((2 * i + 3, 'Y', zi))
        events.sort(key=lambda t: t[0])
        n = 1
        for _, kind, zi in events:
            if kind in 'LR':
                b = (0, zi)
                idx = block(b)
                _remote(buf.at[idx], buf.at[idx], zs.at[zi], zr.at[zi], ep, z).wait_recv()
                if kind == 'L' and z < tps - 1:
                    send(b, buf.at[idx], 'r', ep, z + 1)
                if kind == 'R' and z > 0:
                    send(b, buf.at[idx], 'l', ep, z - 1)
                send(b, buf.at[idx], 'y', across, z)
            else:
                b = (1, zi)
                idx = block(b)
                _remote(buf.at[idx], buf.at[idx], ys.at[zi], yr.at[zi], ep, z).wait_recv()
            send(b, buf.at[idx], 'c', partner, z)
            keep(idx, buf.at[idx], n)
            n += 1
        for same, zi in [(0, zi) for zi in order] + [(1, zi) for zi in order]:
            yy = y if same == 0 else 1 - y
            idx = (yy * 2 + (1 - c)) * tps + zi
            _remote(buf.at[idx], buf.at[idx], cs.at[same * tps + zi], cr.at[same * tps + zi], ep, z).wait_recv()
            keep(idx, buf.at[idx], n)
            n += 1
        for cp in sends:
            cp.wait_send()
        for cp in locals_:
            cp.wait()

    for z in range(tps):
        @pl.when(tp == z)
        def _(z=z):
            body(z)

    for cp in metas:
        cp.wait_send()
    for k in range(1, n_dev):
        src = (me + n_dev - k) % n_dev
        _remote(meta_ref, mall.at[src], ms.at[k], mr.at[k], ep, tp).wait_recv()


def _gather(x, meta, n_dev, tps):
    rows, dim = x.shape
    vmem = pl.BlockSpec(memory_space=pltpu.VMEM)
    dma = pltpu.SemaphoreType.DMA
    return pl.pallas_call(
        functools.partial(_gather_kernel, tps),
        out_shape=(jax.ShapeDtypeStruct((n_dev, rows, dim), x.dtype),
                   jax.ShapeDtypeStruct((n_dev,) + meta.shape, meta.dtype)),
        in_specs=[vmem, vmem],
        out_specs=(pl.BlockSpec(memory_space=pl.ANY), vmem),
        scratch_shapes=[
            pltpu.VMEM((n_dev, rows, dim), x.dtype),
            dma((n_dev,)), dma((n_dev,)), dma((2 * tps,)), dma((tps,)), dma((tps,)), dma((tps,)),
            dma((2 * tps,)), dma((2 * tps,)), dma((n_dev,)),
        ],
        compiler_params=pltpu.CompilerParams(collective_id=0, has_side_effects=True,
                                             vmem_limit_bytes=48 * 1024 * 1024),
    )(x, meta)


NS = 2


def _scatter_kernel(tps, p_hbm, out_ref, own, recd, recy, recr, recl, obuf,
                    ds_, dr, ls, ys, yr, zs, rr, lr):
    ep, tp = lax.axis_index('ep'), lax.axis_index('tp')
    y, c = ep // 2, ep % 2
    partner = y * 2 + (1 - c)
    across = (1 - y) * 2 + c
    rows, dim = out_ref.shape
    cbs = dim // LANES
    blk = rows * cbs
    sub = blk // NS
    step = min(256, sub)

    barrier = pltpu.get_barrier_semaphore()

    def sig(e, t):
        pl.semaphore_signal(barrier, inc=1, device_id={'ep': e, 'tp': t}, device_id_type=pl.DeviceIdType.MESH)

    def accumulate(dst, d0, *srcs):
        @pl.loop(0, sub // step)
        def _(i):
            r = pl.multiple_of(i * step, step)
            v = dst[pl.ds(pl.multiple_of(d0 + r, step), step), :]
            for ref, s0 in srcs:
                v = v + ref[pl.ds(pl.multiple_of(s0 + r, step), step), :]
            dst[pl.ds(pl.multiple_of(d0 + r, step), step), :] = v

    def body(z):
        sig(partner, z)
        sig(across, z)
        if z > 0:
            sig(ep, z - 1)
        if z < tps - 1:
            sig(ep, z + 1)
        pl.semaphore_wait(barrier, 2 + (z > 0) + (z < tps - 1))

        order = {0: [3, 2, 1, 0], 1: [3, 0, 2, 1], 2: [0, 3, 1, 2], 3: [0, 1, 2, 3]}[z]
        sends = []
        work = [(d, s) for d in order for s in range(NS)]

        def off(half, d, s):
            return (half * tps + d) * blk + s * sub

        def sem_i(half, d, s):
            return (half * tps + d) * NS + s

        for half in range(2):
            yy = (1 - y) if half == 0 else y
            for d, s in work:
                i = sem_i(half, d, s)
                src = ((yy * 2 + (1 - c)) * tps + d) * blk + s * sub
                cp = _remote(p_hbm.at[pl.ds(pl.multiple_of(src, sub), sub)], recd.at[pl.ds(off(half, d, s), sub)],
                             ds_.at[i], dr.at[i], partner, z)
                cp.start()
                sends.append(cp)
                src = ((yy * 2 + c) * tps + d) * blk + s * sub
                pltpu.make_async_copy(p_hbm.at[pl.ds(pl.multiple_of(src, sub), sub)],
                                      own.at[pl.ds(off(half, d, s), sub)], ls.at[i]).start()

        def settle(half, d, s):
            i = sem_i(half, d, s)
            o = off(half, d, s)
            here = own.at[pl.ds(o, sub)]
            pltpu.make_async_copy(here, here, ls.at[i]).wait()
            there = recd.at[pl.ds(o, sub)]
            _remote(there, there, ds_.at[i], dr.at[i], partner, z).wait_recv()
            accumulate(own, o, (recd, o))

        for d, s in work:
            settle(0, d, s)
            i = d * NS + s
            cp = _remote(own.at[pl.ds(off(0, d, s), sub)], recy.at[pl.ds(d * blk + s * sub, sub)],
                         ys.at[i], yr.at[i], across, z)
            cp.start()
            sends.append(cp)
        for d, s in work:
            settle(1, d, s)

        for d, s in work:
            i = d * NS + s
            v = d * blk + s * sub
            there = recy.at[pl.ds(v, sub)]
            _remote(there, there, ys.at[i], yr.at[i], across, z).wait_recv()
            o = off(1, d, s)
            srcs = [(recy, v)]
            if z > 0 and d >= z:
                there = recr.at[pl.ds(v, sub)]
                _remote(there, there, zs.at[i], rr.at[i], ep, z).wait_recv()
                srcs.append((recr, v))
            if z < tps - 1 and d <= z:
                there = recl.at[pl.ds(v, sub)]
                _remote(there, there, zs.at[i], lr.at[i], ep, z).wait_recv()
                srcs.append((recl, v))
            if d != z:
                accumulate(own, o, *srcs)
                dst, sem, to = (recr, rr, z + 1) if d > z else (recl, lr, z - 1)
                cp = _remote(own.at[pl.ds(o, sub)], dst.at[pl.ds(v, sub)], zs.at[i], sem.at[i], ep, to)
                cp.start()
                sends.append(cp)
            else:
                per = rows // NS

                @pl.loop(0, per // 16)
                def _(g):
                    for cb in range(cbs):
                        parts = []
                        for hh in range(2):
                            r = g * 16 * cbs + hh * 8 * cbs + cb
                            t = own[pl.ds(o + r, 8, stride=cbs), :]
                            for ref, s0 in srcs:
                                t = t + ref[pl.ds(s0 + r, 8, stride=cbs), :]
                            parts.append(t)
                        w = jnp.concatenate(parts, axis=0).astype(jnp.bfloat16)
                        out_ref[pl.ds(pl.multiple_of(s * per + g * 16, 16), 16), pl.ds(cb * LANES, LANES)] = w
        for cp in sends:
            cp.wait_send()

    for z in range(tps):
        @pl.when(tp == z)
        def _(z=z):
            body(z)


def _scatter(p, rows, dim, tps):
    blk = rows * dim // LANES
    dma = pltpu.SemaphoreType.DMA
    f32 = jnp.float32
    return pl.pallas_call(
        functools.partial(_scatter_kernel, tps),
        out_shape=jax.ShapeDtypeStruct((rows, dim), jnp.bfloat16),
        in_specs=[pl.BlockSpec(memory_space=pl.ANY)],
        out_specs=pl.BlockSpec(memory_space=pltpu.VMEM),
        scratch_shapes=[
            pltpu.VMEM((2 * tps * blk, LANES), f32), pltpu.VMEM((2 * tps * blk, LANES), f32),
            pltpu.VMEM((tps * blk, LANES), f32), pltpu.VMEM((tps * blk, LANES), f32),
            pltpu.VMEM((tps * blk, LANES), f32), pltpu.VMEM((8, LANES), f32),
            dma((2 * tps * NS,)), dma((2 * tps * NS,)), dma((2 * tps * NS,)),
            dma((tps * NS,)), dma((tps * NS,)), dma((tps * NS,)), dma((tps * NS,)), dma((tps * NS,)),
        ],
        compiler_params=pltpu.CompilerParams(collective_id=1, has_side_effects=True,
                                             vmem_limit_bytes=60 * 1024 * 1024),
    )(p)


def solution(mesh):
    tps = mesh.shape['tp']
    n_dev = tps * mesh.shape['ep']

    def expert_block(tok_shard, id_shard, gate_shard, w_gate, w_up, w_down):
        meta = jnp.concatenate([id_shard.T.astype(jnp.float32), gate_shard.T], axis=0)
        x, meta = _gather(tok_shard, meta, n_dev, tps)
        x = x.reshape(n_dev * tok_shard.shape[0], tok_shard.shape[1])
        choices = id_shard.shape[1]
        ids = meta[:, :choices].astype(jnp.int32)
        gates = meta[:, choices:]
        local_count = w_gate.shape[0]
        tok, gate, start = _routing(ids, gates, local_count, lax.axis_index('ep') * local_count)
        y = _moe(tok, gate, start, x, jnp.swapaxes(w_gate, 1, 2), jnp.swapaxes(w_up, 1, 2), w_down)
        return _scatter(y, *tok_shard.shape, tps)

    return jax.shard_map(
        expert_block,
        mesh=mesh,
        in_specs=(P(TOKEN_AXES, None), P(TOKEN_AXES, None), P(TOKEN_AXES, None),
                  P('ep', None, 'tp'), P('ep', None, 'tp'), P('ep', 'tp', None)),
        out_specs=P(TOKEN_AXES, None),
        check_vma=False,
    )
```

```python
import functools

import jax
import jax.numpy as jnp
from jax import lax
from jax.experimental import pallas as pl
from jax.experimental.pallas import tpu as pltpu
from jax.sharding import PartitionSpec as P

TOKEN_AXES = ('dp', 'ep', 'tp')
GROUP_AXES = ('ep', 'tp')
MB = 160
NBUF = 4
LANES = 128
LAG = 3


def _moe_kernel(n_tok, dim, ffp, n_exp, max_blk,
                src_ref, dst_ref, gate_ref, start_ref, x_hbm, wg_hbm, wu_hbm, w2_hbm, y_hbm,
                xf, xst, yacc, wbuf, w2buf, xe, xb0, xb1, h0, h1, o0, o1,
                b_exp, b_base, b_n, b_first, xsem, wsem, ysem):
    cbs = dim // LANES
    tile_rows = cbs * 8
    xc = xst.shape[1]
    n_xc = n_tok // xc
    xb, hb, ob = (xb0, xb1), (h0, h1), (o0, o1)

    def w13(e, slot):
        return (pltpu.make_async_copy(wg_hbm.at[e], wbuf.at[slot, pl.ds(0, ffp)], wsem.at[slot, 0]),
                pltpu.make_async_copy(wu_hbm.at[e], wbuf.at[slot, pl.ds(ffp, ffp)], wsem.at[slot, 1]))

    def w2(e, slot):
        return (pltpu.make_async_copy(w2_hbm.at[e], w2buf.at[slot], wsem.at[slot, 2]),)

    def x_copy(i, slot):
        return pltpu.make_async_copy(x_hbm.at[pl.ds(i * xc, xc)], xst.at[slot], xsem.at[slot])

    x_copy(0, 0).start()
    x_copy(1, 1).start()
    for e in range(NBUF - 1):
        for c in w13(e, e) + w2(e, e):
            c.start()

    def clear(i, carry):
        b_exp[i] = n_exp - 1
        b_base[i] = 0
        b_n[i] = 0
        b_first[i] = 0
        return carry

    lax.fori_loop(0, max_blk, clear, 0)

    def plan(e, at):
        first, last = start_ref[e], start_ref[e + 1]
        pieces = jnp.maximum((last - first + MB - 1) // MB, 1)

        def piece(b, carry):
            b_exp[at + b] = e
            b_base[at + b] = first + b * MB
            b_n[at + b] = jnp.minimum(last - first - b * MB, MB)
            b_first[at + b] = (b == 0).astype(jnp.int32)
            return carry

        lax.fori_loop(0, pieces, piece, 0)
        return at + pieces

    end = lax.fori_loop(0, n_exp, plan, LAG)

    zero = jnp.zeros((tile_rows, LANES), jnp.float32)

    def x_chunk(i, carry):
        slot = lax.rem(i, 2)
        x_copy(i, slot).wait()

        def conv(r, carry2):
            r16 = pl.multiple_of(r * 16, 16)
            row = pl.multiple_of((i * xc + r16) * cbs, 2 * tile_rows)
            for cb in range(cbs):
                v = xst[slot, pl.ds(r16, 16), pl.ds(cb * LANES, LANES)].astype(jnp.float32)
                xf[pl.ds(row + cb * 8, 8), :] = v[:8]
                xf[pl.ds(row + tile_rows + cb * 8, 8), :] = v[8:]
            yacc[pl.ds(row, tile_rows), :] = zero
            yacc[pl.ds(row + tile_rows, tile_rows), :] = zero
            return carry2

        lax.fori_loop(0, xc // 16, conv, 0)

        @pl.when(i + 2 < n_xc)
        def _():
            x_copy(i + 2, slot).start()
        return carry

    lax.fori_loop(0, n_xc, x_chunk, 0)

    def step(i, q):
        j1, j2, j3 = i - 1, i - 2, i - 3
        e1, e2 = b_exp[j1], b_exp[j2]
        s1, s2 = lax.rem(e1, NBUF), lax.rem(e2, NBUF)

        @pl.when(b_first[j1] == 1)
        def _():
            for c in w13(e1, s1):
                c.wait()

            @pl.when(e1 + NBUF - 1 < n_exp)
            def _():
                for c in w13(e1 + NBUF - 1, lax.rem(e1 + NBUF - 1, NBUF)):
                    c.start()

        @pl.when(b_first[j2] == 1)
        def _():
            for c in w2(e2, s2):
                c.wait()

            @pl.when(e2 + NBUF - 1 < n_exp)
            def _():
                for c in w2(e2 + NBUF - 1, lax.rem(e2 + NBUF - 1, NBUF)):
                    c.start()

        base0, base3, n3 = b_base[i], b_base[j3], b_n[j3]

        at = lax.dot_general(wbuf[s1], xb[1 - q][...], (((1,), (1,)), ((), ())),
                             preferred_element_type=jnp.float32)

        h = hb[q][...]
        for nc in range(dim // 256):
            o = jnp.dot(h, w2buf[s2, :, pl.ds(nc * 256, 256)], preferred_element_type=jnp.float32)
            for rb in range(MB // 8):
                for s in range(2):
                    ob[q][pl.ds(rb * tile_rows + (nc * 2 + s) * 8, 8), :] = (
                        o[rb * 8:rb * 8 + 8, s * LANES:(s + 1) * LANES])

        for g in range(MB // 16):
            vals = [xf[pl.ds(src_ref[base0 + g * 16 + k], cbs, stride=8), :] for k in range(16)]
            for k in range(16):
                xe[pl.ds((g * 2 + k // 8) * tile_rows + k % 8, cbs, stride=8), :] = vals[k]
            for cb in range(cbs):
                v = jnp.concatenate([xe[pl.ds(g * 2 * tile_rows + cb * 8, 8), :],
                                     xe[pl.ds((g * 2 + 1) * tile_rows + cb * 8, 8), :]], axis=0)
                xb[q][pl.ds(g * 16, 16), pl.ds(cb * LANES, LANES)] = v.astype(jnp.bfloat16)
            for m in range(2 * g, 2 * g + 2):
                dst, acc = [], []
                for k in range(8):
                    p = m * 8 + k
                    d = pl.multiple_of(jnp.where(p < n3, dst_ref[base3 + p], n_tok * cbs), cbs)
                    dst.append(d)
                    acc.append(yacc[pl.ds(d, cbs), :]
                               + ob[1 - q][pl.ds(m * tile_rows + k, cbs, stride=8), :] * gate_ref[base3 + p])
                for k in range(8):
                    yacc[pl.ds(dst[k], cbs), :] = acc[k]

        ht = jax.nn.silu(at[:ffp]) * at[ffp:]
        hb[1 - q][...] = ht.T.astype(jnp.bfloat16)

    def pair(t, carry):
        step(LAG + 2 * t, 0)
        step(LAG + 2 * t + 1, 1)
        return carry

    lax.fori_loop(0, (end + 1) // 2, pair, 0)
    out = pltpu.make_async_copy(yacc.at[pl.ds(0, n_tok * cbs)], y_hbm, ysem)
    out.start()
    out.wait()


def _moe(src, dst, gate, start, x, wgt, wut, w2):
    n_exp, ffp, dim = wgt.shape
    n_tok = x.shape[0]
    cbs = dim // LANES
    n_pairs = src.shape[0] - MB
    max_blk = n_exp + n_pairs // MB + 2 * LAG + 4
    smem = pl.BlockSpec(memory_space=pltpu.SMEM)
    hbm = pl.BlockSpec(memory_space=pl.ANY)
    f32, bf16 = jnp.float32, jnp.bfloat16
    return pl.pallas_call(
        functools.partial(_moe_kernel, n_tok, dim, ffp, n_exp, max_blk),
        out_shape=jax.ShapeDtypeStruct((n_tok * cbs, LANES), jnp.float32),
        in_specs=[smem, smem, smem, smem, hbm, hbm, hbm, hbm],
        out_specs=hbm,
        scratch_shapes=[
            pltpu.VMEM((n_tok * cbs, LANES), f32),
            pltpu.VMEM((2, 128, dim), bf16),
            pltpu.VMEM(((n_tok + 8) * cbs, LANES), f32),
            pltpu.VMEM((NBUF, 2 * ffp, dim), bf16),
            pltpu.VMEM((NBUF, ffp, dim), bf16),
            pltpu.VMEM((MB * cbs, LANES), f32),
            pltpu.VMEM((MB, dim), bf16), pltpu.VMEM((MB, dim), bf16),
            pltpu.VMEM((MB, ffp), bf16), pltpu.VMEM((MB, ffp), bf16),
            pltpu.VMEM((MB * cbs, LANES), f32), pltpu.VMEM((MB * cbs, LANES), f32),
            pltpu.SMEM((max_blk,), jnp.int32), pltpu.SMEM((max_blk,), jnp.int32),
            pltpu.SMEM((max_blk,), jnp.int32), pltpu.SMEM((max_blk,), jnp.int32),
            pltpu.SemaphoreType.DMA((2,)),
            pltpu.SemaphoreType.DMA((NBUF, 3)),
            pltpu.SemaphoreType.DMA,
        ],
        compiler_params=pltpu.CompilerParams(vmem_limit_bytes=62 * 1024 * 1024),
        cost_estimate=pl.CostEstimate(flops=20_000_000_000, bytes_accessed=100_000_000, transcendentals=1_000_000),
    )(src, dst, gate, start, x, wgt, wut, w2)


def _routing(ids, gates, local_count, first_expert, cbs):
    devs, choices, rows = ids.shape
    n_tok = devs * rows
    tok = (lax.broadcasted_iota(jnp.int32, ids.shape, 0) * rows
           + lax.broadcasted_iota(jnp.int32, ids.shape, 2))
    local = ids - first_expert
    key = jnp.where((local >= 0) & (local < local_count), local * n_tok + tok, local_count * n_tok)
    key = key.reshape(-1)
    n_pairs = key.shape[0] // 4
    bounds = jnp.arange(local_count + 1, dtype=jnp.int32) * n_tok
    start = jnp.sum((key[None, :] < bounds[:, None]).astype(jnp.int32), axis=1)
    key_s, gate_s = lax.sort((key, gates.reshape(-1)), num_keys=1, is_stable=False)
    tok_s = key_s[:n_pairs + MB] & (n_tok - 1)
    src = (tok_s >> 3) * (8 * cbs) + (tok_s & 7)
    return src, tok_s * cbs, gate_s[:n_pairs + MB], start


def _wire(ep, tp):
    return ep // 2, ep % 2


def _remote(src, dst, send, recv, ep, tp):
    return pltpu.make_async_remote_copy(src_ref=src, dst_ref=dst, send_sem=send, recv_sem=recv,
                                        device_id={'ep': ep, 'tp': tp},
                                        device_id_type=pl.DeviceIdType.MESH)


def _gather_kernel(tps, x_ref, meta_ref, xall, mall, buf, ms, mr, zs, zr, ys, yr, cs, cr, ls):
    ep, tp = lax.axis_index('ep'), lax.axis_index('tp')
    n_dev = mall.shape[0]
    y, c = ep // 2, ep % 2
    me = ep * tps + tp
    partner = y * 2 + (1 - c)
    across = (1 - y) * 2 + c

    barrier = pltpu.get_barrier_semaphore()
    for k in range(1, n_dev):
        peer = (me + k) % n_dev
        pl.semaphore_signal(barrier, inc=1, device_id={'ep': peer // tps, 'tp': peer % tps},
                            device_id_type=pl.DeviceIdType.MESH)
    pl.semaphore_wait(barrier, n_dev - 1)

    metas = []
    for k in range(1, n_dev):
        peer = (me + k) % n_dev
        cp = _remote(meta_ref, mall.at[me], ms.at[k], mr.at[k], peer // tps, peer % tps)
        cp.start()
        metas.append(cp)
    mall[pl.ds(me, 1)] = meta_ref[...][None]

    def body(z):
        sends = []

        def send(b, src, kind, ep_to, tp_to):
            s, r = {'r': (zs, zr), 'l': (zs, zr), 'y': (ys, yr), 'c': (cs, cr)}[kind]
            zi = b[1]
            si = {'r': zi, 'l': tps + zi, 'y': zi, 'c': b[0] * tps + zi}[kind]
            row = (b[0] if kind != 'c' else b[0])
            idx = block(b)
            cp = _remote(src, buf.at[idx], s.at[si], r.at[zi if kind in 'rly' else si], ep_to, tp_to)
            cp.start()
            sends.append(cp)

        def block(b):
            yy = y if b[0] == 0 else 1 - y
            return (yy * 2 + c) * tps + b[1]

        def keep(idx, src, n):
            cp = pltpu.make_async_copy(src, xall.at[idx], ls.at[n])
            cp.start()
            locals_.append(cp)

        locals_ = []
        own = block((0, z))
        if z < tps - 1:
            send((0, z), x_ref, 'r', ep, z + 1)
        if z > 0:
            send((0, z), x_ref, 'l', ep, z - 1)
        send((0, z), x_ref, 'y', across, z)
        send((0, z), x_ref, 'c', partner, z)
        keep(own, x_ref, 0)

        events = []
        order = [z]
        for dist in range(1, tps):
            if z - dist >= 0:
                events.append((dist * 2, 'L', z - dist))
                order.append(z - dist)
            if z + dist < tps:
                events.append((dist * 2, 'R', z + dist))
                order.append(z + dist)
        for i, zi in enumerate(order):
            events.append((2 * i + 3, 'Y', zi))
        events.sort(key=lambda t: t[0])
        n = 1
        for _, kind, zi in events:
            if kind in 'LR':
                b = (0, zi)
                idx = block(b)
                _remote(buf.at[idx], buf.at[idx], zs.at[zi], zr.at[zi], ep, z).wait_recv()
                if kind == 'L' and z < tps - 1:
                    send(b, buf.at[idx], 'r', ep, z + 1)
                if kind == 'R' and z > 0:
                    send(b, buf.at[idx], 'l', ep, z - 1)
                send(b, buf.at[idx], 'y', across, z)
            else:
                b = (1, zi)
                idx = block(b)
                _remote(buf.at[idx], buf.at[idx], ys.at[zi], yr.at[zi], ep, z).wait_recv()
            send(b, buf.at[idx], 'c', partner, z)
            keep(idx, buf.at[idx], n)
            n += 1
        for same, zi in [(0, zi) for zi in order] + [(1, zi) for zi in order]:
            yy = y if same == 0 else 1 - y
            idx = (yy * 2 + (1 - c)) * tps + zi
            _remote(buf.at[idx], buf.at[idx], cs.at[same * tps + zi], cr.at[same * tps + zi], ep, z).wait_recv()
            keep(idx, buf.at[idx], n)
            n += 1
        for cp in sends:
            cp.wait_send()
        for cp in locals_:
            cp.wait()

    for z in range(tps):
        @pl.when(tp == z)
        def _(z=z):
            body(z)

    for cp in metas:
        cp.wait_send()
    for k in range(1, n_dev):
        src = (me + n_dev - k) % n_dev
        _remote(meta_ref, mall.at[src], ms.at[k], mr.at[k], ep, tp).wait_recv()


def _gather(x, meta, n_dev, tps):
    rows, dim = x.shape
    vmem = pl.BlockSpec(memory_space=pltpu.VMEM)
    dma = pltpu.SemaphoreType.DMA
    return pl.pallas_call(
        functools.partial(_gather_kernel, tps),
        out_shape=(jax.ShapeDtypeStruct((n_dev, rows, dim), x.dtype),
                   jax.ShapeDtypeStruct((n_dev,) + meta.shape, meta.dtype)),
        in_specs=[vmem, vmem],
        out_specs=(pl.BlockSpec(memory_space=pl.ANY), vmem),
        scratch_shapes=[
            pltpu.VMEM((n_dev, rows, dim), x.dtype),
            dma((n_dev,)), dma((n_dev,)), dma((2 * tps,)), dma((tps,)), dma((tps,)), dma((tps,)),
            dma((2 * tps,)), dma((2 * tps,)), dma((n_dev,)),
        ],
        compiler_params=pltpu.CompilerParams(collective_id=0, has_side_effects=True,
                                             vmem_limit_bytes=48 * 1024 * 1024),
    )(x, meta)


NS = 2


def _scatter_kernel(tps, p_hbm, out_ref, own, recd, recy, recr, recl, obuf,
                    ds_, dr, ls, ys, yr, zs, rr, lr):
    ep, tp = lax.axis_index('ep'), lax.axis_index('tp')
    y, c = ep // 2, ep % 2
    partner = y * 2 + (1 - c)
    across = (1 - y) * 2 + c
    rows, dim = out_ref.shape
    cbs = dim // LANES
    blk = rows * cbs
    sub = blk // NS
    step = min(256, sub)

    barrier = pltpu.get_barrier_semaphore()

    def sig(e, t):
        pl.semaphore_signal(barrier, inc=1, device_id={'ep': e, 'tp': t}, device_id_type=pl.DeviceIdType.MESH)

    def accumulate(dst, d0, *srcs):
        @pl.loop(0, sub // step)
        def _(i):
            r = pl.multiple_of(i * step, step)
            v = dst[pl.ds(pl.multiple_of(d0 + r, step), step), :]
            for ref, s0 in srcs:
                v = v + ref[pl.ds(pl.multiple_of(s0 + r, step), step), :]
            dst[pl.ds(pl.multiple_of(d0 + r, step), step), :] = v

    def body(z):
        sig(partner, z)
        sig(across, z)
        if z > 0:
            sig(ep, z - 1)
        if z < tps - 1:
            sig(ep, z + 1)
        pl.semaphore_wait(barrier, 2 + (z > 0) + (z < tps - 1))

        order = {0: [3, 2, 1, 0], 1: [3, 0, 2, 1], 2: [0, 3, 1, 2], 3: [0, 1, 2, 3]}[z]
        sends = []
        work = [(d, s) for d in order for s in range(NS)]

        def off(half, d, s):
            return (half * tps + d) * blk + s * sub

        def sem_i(half, d, s):
            return (half * tps + d) * NS + s

        for half in range(2):
            yy = (1 - y) if half == 0 else y
            for d, s in work:
                i = sem_i(half, d, s)
                src = ((yy * 2 + (1 - c)) * tps + d) * blk + s * sub
                cp = _remote(p_hbm.at[pl.ds(pl.multiple_of(src, sub), sub)], recd.at[pl.ds(off(half, d, s), sub)],
                             ds_.at[i], dr.at[i], partner, z)
                cp.start()
                sends.append(cp)
                src = ((yy * 2 + c) * tps + d) * blk + s * sub
                pltpu.make_async_copy(p_hbm.at[pl.ds(pl.multiple_of(src, sub), sub)],
                                      own.at[pl.ds(off(half, d, s), sub)], ls.at[i]).start()

        def settle(half, d, s):
            i = sem_i(half, d, s)
            o = off(half, d, s)
            here = own.at[pl.ds(o, sub)]
            pltpu.make_async_copy(here, here, ls.at[i]).wait()
            there = recd.at[pl.ds(o, sub)]
            _remote(there, there, ds_.at[i], dr.at[i], partner, z).wait_recv()
            accumulate(own, o, (recd, o))

        for d, s in work:
            settle(0, d, s)
            i = d * NS + s
            cp = _remote(own.at[pl.ds(off(0, d, s), sub)], recy.at[pl.ds(d * blk + s * sub, sub)],
                         ys.at[i], yr.at[i], across, z)
            cp.start()
            sends.append(cp)
        for d, s in work:
            settle(1, d, s)

        for d, s in work:
            i = d * NS + s
            v = d * blk + s * sub
            there = recy.at[pl.ds(v, sub)]
            _remote(there, there, ys.at[i], yr.at[i], across, z).wait_recv()
            o = off(1, d, s)
            srcs = [(recy, v)]
            if z > 0 and d >= z:
                there = recr.at[pl.ds(v, sub)]
                _remote(there, there, zs.at[i], rr.at[i], ep, z).wait_recv()
                srcs.append((recr, v))
            if z < tps - 1 and d <= z:
                there = recl.at[pl.ds(v, sub)]
                _remote(there, there, zs.at[i], lr.at[i], ep, z).wait_recv()
                srcs.append((recl, v))
            if d != z:
                accumulate(own, o, *srcs)
                dst, sem, to = (recr, rr, z + 1) if d > z else (recl, lr, z - 1)
                cp = _remote(own.at[pl.ds(o, sub)], dst.at[pl.ds(v, sub)], zs.at[i], sem.at[i], ep, to)
                cp.start()
                sends.append(cp)
            else:
                per = rows // NS

                @pl.loop(0, per // 16)
                def _(g):
                    for cb in range(cbs):
                        parts = []
                        for hh in range(2):
                            r = g * 16 * cbs + hh * 8 * cbs + cb
                            t = own[pl.ds(o + r, 8, stride=cbs), :]
                            for ref, s0 in srcs:
                                t = t + ref[pl.ds(s0 + r, 8, stride=cbs), :]
                            parts.append(t)
                        w = jnp.concatenate(parts, axis=0).astype(jnp.bfloat16)
                        out_ref[pl.ds(pl.multiple_of(s * per + g * 16, 16), 16), pl.ds(cb * LANES, LANES)] = w
        for cp in sends:
            cp.wait_send()

    for z in range(tps):
        @pl.when(tp == z)
        def _(z=z):
            body(z)


def _scatter(p, rows, dim, tps):
    blk = rows * dim // LANES
    dma = pltpu.SemaphoreType.DMA
    f32 = jnp.float32
    return pl.pallas_call(
        functools.partial(_scatter_kernel, tps),
        out_shape=jax.ShapeDtypeStruct((rows, dim), jnp.bfloat16),
        in_specs=[pl.BlockSpec(memory_space=pl.ANY)],
        out_specs=pl.BlockSpec(memory_space=pltpu.VMEM),
        scratch_shapes=[
            pltpu.VMEM((2 * tps * blk, LANES), f32), pltpu.VMEM((2 * tps * blk, LANES), f32),
            pltpu.VMEM((tps * blk, LANES), f32), pltpu.VMEM((tps * blk, LANES), f32),
            pltpu.VMEM((tps * blk, LANES), f32), pltpu.VMEM((8, LANES), f32),
            dma((2 * tps * NS,)), dma((2 * tps * NS,)), dma((2 * tps * NS,)),
            dma((tps * NS,)), dma((tps * NS,)), dma((tps * NS,)), dma((tps * NS,)), dma((tps * NS,)),
        ],
        compiler_params=pltpu.CompilerParams(collective_id=1, has_side_effects=True,
                                             vmem_limit_bytes=60 * 1024 * 1024),
    )(p)


def solution(mesh):
    tps = mesh.shape['tp']
    n_dev = tps * mesh.shape['ep']

    def expert_block(tok_shard, id_shard, gate_shard, w_gate, w_up, w_down):
        meta = jnp.concatenate([id_shard.T.astype(jnp.float32), gate_shard.T], axis=0)
        x, meta = _gather(tok_shard, meta, n_dev, tps)
        x = x.reshape(n_dev * tok_shard.shape[0], tok_shard.shape[1])
        choices = id_shard.shape[1]
        ids = meta[:, :choices].astype(jnp.int32)
        gates = meta[:, choices:]
        local_count = w_gate.shape[0]
        src, dst, gate, start = _routing(ids, gates, local_count, lax.axis_index('ep') * local_count,
                                         tok_shard.shape[1] // LANES)
        y = _moe(src, dst, gate, start, x, jnp.swapaxes(w_gate, 1, 2), jnp.swapaxes(w_up, 1, 2), w_down)
        return _scatter(y, *tok_shard.shape, tps)

    return jax.shard_map(
        expert_block,
        mesh=mesh,
        in_specs=(P(TOKEN_AXES, None), P(TOKEN_AXES, None), P(TOKEN_AXES, None),
                  P('ep', None, 'tp'), P('ep', None, 'tp'), P('ep', 'tp', None)),
        out_specs=P(TOKEN_AXES, None),
        check_vma=False,
    )
```
